32 devices in a mesh: rep: 2 (over z, core), dp: 16 (over x, y).
Axes of the slice: x: 4, y: 4, z: 1, core: 2. Of those that a mesh axis runs over, the one named last changes fastest.
The devices are a block of a 4x4x8 slice.
Arguments:
- x: bfloat16 [32, 4096, 768], P(('rep', 'dp')), parts along dimension 0
- dy: bfloat16 [32, 4096, 768], P(('rep', 'dp')), parts along dimension 0
- w_gate: bfloat16 [2, 768, 1792], P(None, 'dp')
- w_up: bfloat16 [2, 768, 1792], P(None, 'dp')
- w_down: bfloat16 [2, 1792, 768], P(None, 'dp')
- m_w_gate: float32 [2, 768, 1792], P(None, 'dp')
- m_w_up: float32 [2, 768, 1792], P(None, 'dp')
- m_w_down: float32 [2, 1792, 768], P(None, 'dp')
- v_w_gate: float32 [2, 768, 1792], P(None, 'dp')
- v_w_up: float32 [2, 768, 1792], P(None, 'dp')
- v_w_down: float32 [2, 1792, 768], P(None, 'dp')
Outputs:
- output 1: bfloat16 [4, 768, 1792], P('rep', 'dp'), parts along dimension 0
- output 2: bfloat16 [4, 768, 1792], P('rep', 'dp'), parts along dimension 0
- output 3: bfloat16 [4, 1792, 768], P('rep', 'dp'), parts along dimension 0
- output 4: float32 [4, 768, 1792], P('rep', 'dp'), parts along dimension 0
- output 5: float32 [4, 768, 1792], P('rep', 'dp'), parts along dimension 0
- output 6: float32 [4, 1792, 768], P('rep', 'dp'), parts along dimension 0
- output 7: float32 [4, 768, 1792], P('rep', 'dp'), parts along dimension 0
- output 8: float32 [4, 768, 1792], P('rep', 'dp'), parts along dimension 0
- output 9: float32 [4, 1792, 768], P('rep', 'dp'), parts along dimension 0
There are 2 independent parts. The reference program is written for one: setup_inputs(seed, part) draws one part's arguments, and reference() takes and returns one part's arrays. A program takes and returns all parts, laid end to end along the dimension named above; an argument that names none is the same for every part.
All inputs are finite; a program needn't handle non-finite values.
Results may differ from the reference program's by a relative error of at most 0.022.
Values are sent between devices in bfloat16 or wider.
A program may use at most 768 MiB of HBM per device.

```python
import jax
import jax.numpy as jnp
from jax import lax

SEQUENCES = 16
TOKENS = 4096
D = 768
FF = 1792
LAYERS = 2
NAMES = ("w_gate", "w_up", "w_down")
SHAPES = {"w_gate": (LAYERS, D, FF), "w_up": (LAYERS, D, FF), "w_down": (LAYERS, FF, D)}


def bump(key, n, height):
    away = (jnp.arange(n, dtype=jnp.int32) - jax.random.randint(key, (), 0, n, jnp.int32)) % n
    return jnp.where(away < n // 8, height, 1.0)


def together(key, own, strength):
    shared = jax.random.normal(key, own.shape[1:], jnp.float32)
    return (own + strength * shared) * lax.rsqrt(1 + strength * strength)


def setup_inputs(seed: int = 0, part: int = 0) -> dict:
    kx, kdy, ka, kb, kz, kf, kh, kl, *keys = jax.random.split(jax.random.key(seed), 8 + 3 * len(NAMES))
    kx, kdy, ka, kb = (jax.random.fold_in(k, part) for k in (kx, kdy, ka, kb))
    kw, km, kv = (keys[i::3] for i in range(3))
    shape = (SEQUENCES, TOKENS, D)
    much_x, much_dy = jax.random.uniform(kz, (2,), jnp.float32, 0.0, 1.0)
    loud = 2.0 ** jax.random.uniform(jax.random.fold_in(kz, 1), (), jnp.float32, -1.0, 2.0)
    layers = 2.0 ** jax.random.uniform(kl, (LAYERS, 1, 1), jnp.float32, -1.0, 1.0)
    x = together(ka, jax.random.normal(kx, shape, jnp.float32), much_x) * bump(kf, D, 4.0)
    dy = together(kb, jax.random.normal(kdy, shape, jnp.float32), much_dy)
    drawn = {"x": x.astype(jnp.bfloat16), "dy": (loud * dy * (SEQUENCES * TOKENS) ** -0.5).astype(jnp.bfloat16)}
    for key, name in zip(kw, NAMES, strict=True):
        w = jax.random.normal(key, SHAPES[name], jnp.float32) * SHAPES[name][1] ** -0.5
        drawn[name] = (w * {"w_gate": 1.0, "w_up": bump(kh, FF, 4.0), "w_down": layers}[name]).astype(jnp.bfloat16)
    for key, name in zip(km, NAMES, strict=True):
        drawn[f"m_{name}"] = 0.1 * jax.random.normal(key, SHAPES[name], jnp.float32)
    for key, name in zip(kv, NAMES, strict=True):
        drawn[f"v_{name}"] = jax.random.uniform(key, SHAPES[name], jnp.float32, 0.005, 0.015)
    return drawn


def matmul(a, w):
    return jnp.dot(a, w, preferred_element_type=jnp.float32).astype(jnp.bfloat16)


def normed(h):
    wide = h.astype(jnp.float32)
    scale = lax.rsqrt(jnp.mean(wide**2, -1, keepdims=True) + 1e-6)
    return (wide * scale).astype(jnp.bfloat16)


def layer(h, w):
    a = normed(h)
    gate = jnp.dot(a, w["w_gate"], preferred_element_type=jnp.float32)
    up = jnp.dot(a, w["w_up"], preferred_element_type=jnp.float32)
    return h + matmul((jax.nn.silu(gate) * up).astype(jnp.bfloat16), w["w_down"])


def adamw(w, m, v, g):
    m = 0.9 * m + 0.1 * g
    v = 0.95 * v + 0.05 * g * g
    step = m * lax.rsqrt(v + 1e-8) + 0.1 * w
    return (w - 0.02 * step).astype(jnp.bfloat16), m, v


def clipped(gradients, sum_of_squares, count):
    factor = jnp.minimum(1.0, 0.5 * lax.rsqrt(sum_of_squares / count + 1e-30))
    return [g * factor for g in gradients]


def stack(weights, h):
    return lax.scan(lambda h, w: (layer(h, w), None), h, weights)[0]


def reference(x, dy, w_gate, w_up, w_down, m_w_gate, m_w_up, m_w_down, v_w_gate, v_w_up, v_w_down):
    weights = dict(zip(NAMES, (w_gate, w_up, w_down), strict=True))

    def take(so_far, sequence):
        h, by_y = sequence
        _, back = jax.vjp(lambda w: stack(w, h), weights)
        return jax.tree.map(lambda total, term: total + term.astype(jnp.float32), so_far, back(by_y)[0]), None

    none_yet = {name: jnp.zeros(w.shape, jnp.float32) for name, w in weights.items()}
    by_weights, _ = lax.scan(take, none_yet, (x, dy))
    gradients = [by_weights[name].astype(jnp.bfloat16).astype(jnp.float32) for name in NAMES]
    gradients = clipped(gradients, sum(jnp.sum(g * g) for g in gradients), sum(g.size for g in gradients))
    new = [
        adamw(w.astype(jnp.float32), m, v, g)
        for w, m, v, g in zip((w_gate, w_up, w_down), (m_w_gate, m_w_up, m_w_down), (v_w_gate, v_w_up, v_w_down), gradients, strict=True)
    ]
    return tuple(one[which] for which in range(3) for one in new)
```

```python
import functools
import math

import jax
import jax.numpy as jnp
from jax import lax
from jax.experimental import pallas as pl
from jax.experimental.pallas import tpu as pltpu
from jax.sharding import PartitionSpec as P

BF16, F32 = jnp.bfloat16, jnp.float32
LANES = 128
CHUNK = 2 * LANES
TILE = 256
UNROLL = 4
SPAN = TILE * UNROLL
WIDE = 512
EPS = 1e-6
BOTH = (0, 1)
ANY = pl.BlockSpec(memory_space=pl.ANY)
VMEM = pl.BlockSpec(memory_space=pltpu.VMEM)
MESH_IDS = pl.DeviceIdType.MESH
VMEM_LIMIT = 67_000_000


def dot(a, b):
    return jnp.dot(a, b, preferred_element_type=F32)


def dot_nt(a, b):
    return lax.dot_general(a, b, (((1,), (1,)), ((), ())), preferred_element_type=F32)


def rounded(x):
    return x.astype(BF16).astype(F32)


def aligned(start, size):
    return pl.ds(pl.multiple_of(start, size), size)


def local(src, dst, sem):
    return pltpu.make_async_copy(src, dst, sem)


def loop(n, body):
    def step(i, carry):
        body(i)
        return carry

    lax.fori_loop(0, n, step, 0)


class Torus:
    def __init__(self, side):
        index = lax.axis_index("dp")
        self.side = side
        self.at = (index // side, lax.rem(index, side))

    def near(self, axis, away):
        return lax.rem(self.at[axis] + away + self.side, self.side)

    def id(self, axis, away):
        place = [self.at[0], self.at[1]]
        place[axis] = self.near(axis, away)
        return {"dp": place[0] * self.side + place[1]}

    def partner(self):
        rep = lax.axis_index("rep")
        return {"rep": rep + 1 - 2 * lax.rem(rep, 2)}

    def greet(self, targets):
        barrier = pltpu.get_barrier_semaphore()
        for target in targets:
            pl.semaphore_signal(barrier, inc=1, device_id=target, device_id_type=MESH_IDS)
        pl.semaphore_wait(barrier, len(targets))


def remote(src, dst, send, recv, target):
    return pltpu.make_async_remote_copy(src_ref=src, dst_ref=dst, send_sem=send, recv_sem=recv, device_id=target, device_id_type=MESH_IDS)


class Gather:
    def __init__(self, torus, full, own, sems):
        self.t, self.full, self.own, self.send, self.recv = torus, full, own, sems.at[0], sems.at[1]
        self.core = lax.rem(lax.axis_index("rep"), 2)

    def cols(self, piece):
        return aligned(piece * CHUNK + self.core * LANES, LANES)

    def copy(self, k, which, src, dst, target):
        return remote(src, dst, self.send.at[k, which], self.recv.at[k, which], target)

    def block(self, axis, along, piece):
        i = (along, self.t.at[1]) if axis == 0 else (self.t.at[0], along)
        return self.full.at[i[0], i[1], :, self.cols(piece)]

    def line(self, axis, across, piece):
        c = self.cols(piece)
        return self.full.at[:, across, :, c] if axis == 0 else self.full.at[across, :, :, c]

    def near_pair(self, k, piece, axis):
        b = self.block(axis, self.t.at[axis], piece)
        own = self.own.at[:, self.cols(piece)]
        return [self.copy(k, n, own, b, self.t.id(axis, 1 - 2 * n)) for n in BOTH]

    def far_block(self, k, piece, axis, odd):
        b = self.block(axis, self.t.near(axis, 2 * odd - 1), piece)
        return self.copy(k, 2, b, b, self.t.id(axis, 1 - 2 * odd))

    def line_pair(self, k, piece, axis):
        mine = self.line(axis, self.t.at[1 - axis], piece)
        return [self.copy(k, 3 + n, mine, mine, self.t.id(1 - axis, 1 - 2 * n)) for n in BOTH]

    def far_line(self, k, piece, axis, odd):
        line = self.line(axis, self.t.near(1 - axis, 2 * odd - 1), piece)
        return self.copy(k, 5, line, line, self.t.id(1 - axis, 1 - 2 * odd))

    def across(self, k, piece):
        whole = self.full.at[:, :, :, self.cols(piece)]
        return self.copy(k, 6, whole, whole, self.t.partner())

    def wait(self, k, which, like):
        self.copy(k, which, like, like, self.t.partner()).wait_recv()

    def stage(self, n, k, piece, axis, odd):
        block = self.block(axis, self.t.at[axis], piece)
        line = self.line(axis, self.t.at[1 - axis], piece)
        if n == 0:
            for c in self.near_pair(k, piece, axis):
                c.start()
        elif n == 1:
            self.wait(k, odd, block)
            self.far_block(k, piece, axis, odd).start()
        elif n == 2:
            self.wait(k, 1 - odd, block)
            self.wait(k, 2, block)
            for c in self.line_pair(k, piece, axis):
                c.start()
        elif n == 3:
            self.wait(k, 3 + odd, line)
            self.far_line(k, piece, axis, odd).start()
        elif n == 4:
            self.wait(k, 4 - odd, line)
            self.wait(k, 5, line)
            self.across(k, piece).start()
        elif n == 5:
            self.wait(k, 6, self.full.at[:, :, :, self.cols(piece)])
        else:
            for c in self.near_pair(k, piece, axis) + self.line_pair(k, piece, axis):
                c.wait_send()
            self.far_block(k, piece, axis, odd).wait_send()
            self.far_line(k, piece, axis, odd).wait_send()
            self.across(k, piece).wait_send()


class Scatter:
    def __init__(self, torus, rows, refs):
        self.t, self.rows = torus, rows
        self.sa, self.ra, self.sb, self.rb, self.q, self.sems = refs

    @staticmethod
    def scratch(side, rows, pieces, slots):
        return [
            pltpu.VMEM((slots, 3, side, rows, LANES), BF16),
            pltpu.VMEM((pieces, 3, side, rows, LANES), BF16),
            pltpu.VMEM((slots, 3, rows, LANES), BF16),
            pltpu.VMEM((pieces, 3, rows, LANES), BF16),
            pltpu.VMEM((slots, side, rows, LANES), F32),
            pltpu.SemaphoreType.DMA((pieces, 2, 2, 3)),
        ]

    def copy(self, phase, k, slot, which, axis, way):
        src, dst = ((self.sa, self.ra), (self.sb, self.rb))[phase]
        if phase:
            axis = 1 - axis
        target = self.t.id(axis, -way if which == 1 else way)
        sems = self.sems.at[k, phase]
        return remote(src.at[slot, which], dst.at[k, which], sems.at[0, which], sems.at[1, which], target)

    def stage(self, n, k, slot, axis, way, own, out):
        t, side, other = self.t, self.t.side, 1 - axis

        def term(along, across):
            return own(along, across) if axis == 0 else own(across, along)

        if n == 0:
            for which, away in ((0, 2), (1, -way)):
                for i in range(side):
                    self.sa[slot, which, i] = term(t.near(axis, away), i).astype(BF16)
                self.copy(0, k, slot, which, axis, way).start()
        elif n == 1:
            self.copy(0, k, slot, 0, axis, way).wait_recv()
            for i in range(side):
                self.sa[slot, 2, i] = (term(t.near(axis, way), i) + self.ra[k, 0, i].astype(F32)).astype(BF16)
            self.copy(0, k, slot, 2, axis, way).start()
        elif n == 2:
            for which in (1, 2):
                self.copy(0, k, slot, which, axis, way).wait_recv()
            for i in range(side):
                self.q[slot, i] = term(t.at[axis], i) + self.ra[k, 1, i].astype(F32) + self.ra[k, 2, i].astype(F32)
            for which, away in ((0, 2), (1, -way)):
                self.sb[slot, which] = self.q[slot, t.near(other, away)].astype(BF16)
                self.copy(1, k, slot, which, axis, way).start()
        elif n == 3:
            self.copy(1, k, slot, 0, axis, way).wait_recv()
            self.sb[slot, 2] = (self.q[slot, t.near(other, way)] + self.rb[k, 0].astype(F32)).astype(BF16)
            self.copy(1, k, slot, 2, axis, way).start()
        else:
            for which in (1, 2):
                self.copy(1, k, slot, which, axis, way).wait_recv()
            out(self.q[slot, t.at[other]] + self.rb[k, 1].astype(F32) + self.rb[k, 2].astype(F32))
            for phase in BOTH:
                for which in range(3):
                    self.copy(phase, k, slot, which, axis, way).wait_send()


def greeted(t, aways):
    return [t.id(axis, away) for axis in BOTH for away in aways]


def scale_of(wide):
    return lax.rsqrt(jnp.mean(wide * wide, -1, keepdims=True) + EPS)


def normed(h):
    wide = h.astype(F32)
    return (wide * scale_of(wide)).astype(BF16)


def front_kernel(side, x, dy, wg, wu, wd, ao, bo, po, a0t, dyt, ho, a1, a1t, wd0o, wg1, wu1, wd1, vx, va, vp, vg, vu, vd, ab, td, tt, th, ta, xsem, psem, asem, sem, *gather_sems):
    t = Torus(side)
    tokens, ff = vp.shape
    d = vx.shape[1]
    chunks, dchunks, blocks, spans = ff // CHUNK, d // CHUNK, tokens // WIDE, tokens // SPAN
    me = t.at

    def rows_of(b):
        return aligned(b * WIDE, WIDE)

    def xin(b):
        return local(x.at[rows_of(b)], vx.at[rows_of(b)], xsem.at[b])

    loop(blocks, lambda b: xin(b).start())
    for full, shard in ((vg, wg), (vu, wu), (vd, wd)):
        full[me[0], me[1]] = shard[0]
    own1 = [local(s.at[1], o.at[me[0], me[1]], psem.at[i]) for i, (s, o) in enumerate(((wg, wg1), (wu, wu1), (wd, wd1)))]
    for c in own1:
        c.start()
    t.greet([*greeted(t, (1, -1)), t.partner()])

    shards, layers = (wg, wu, wd), ((vg, vu, vd), (wg1, wu1, wd1))
    gathers = [[Gather(t, f, s.at[n], gather_sems[3 * n + i]) for i, (f, s) in enumerate(zip(fulls, shards))] for n, fulls in enumerate(layers)]

    def wide(layer, n, c):
        for axis in BOTH:
            gathers[layer][axis].stage(n, c, c, axis, lax.rem(c, 2))

    def tall(layer, n):
        for c in range(dchunks):
            gathers[layer][2].stage(n, c, c, (c + layer) % 2, (c // 2 + layer) % 2)

    def all_wide(layer, n):
        loop(chunks, lambda c: wide(layer, n, c))

    def due(i, plan):
        for at, *work in plan:

            @pl.when(i == at)
            def _(work=work):
                for f, *args in work:
                    f(*args)

    all_wide(0, 0)

    def turned(dst, b):
        slot = lax.rem(b, 2)
        return local(tt.at[slot], dst.at[:, rows_of(b)], sem.at[slot])

    def turn(dst, plan, get):
        def block(b):
            @pl.when(b >= 2)
            def _():
                turned(dst, b).wait()

            for q in range(0, WIDE, LANES):
                tt[lax.rem(b, 2), :, pl.ds(q, LANES)] = get(b, q).T
            turned(dst, b).start()
            due(b, plan)

        loop(blocks, block)
        for b in BOTH:
            turned(dst, b).wait()

    def first_states(b, q):
        if q == 0:
            xin(b).wait()
        r = aligned(b * WIDE + q, LANES)
        a = normed(vx[r, :])
        va[r, :] = a
        return a

    def dyin(b):
        slot = lax.rem(b, 2)
        return local(dy.at[rows_of(b)], td.at[slot], sem.at[2 + slot])

    def cotangent(b, q):
        if q == 0:

            @pl.when(b + 1 < blocks)
            def _():
                dyin(b + 1).start()

            dyin(b).wait()
        return td[lax.rem(b, 2), pl.ds(q, LANES), :]

    dyin(0).start()
    turn(a0t, ((2, (all_wide, 0, 1)), (6, (all_wide, 0, 2), (tall, 0, 0))), first_states)
    turn(dyt, ((2, (wide, 0, 3, 0)), (6, (wide, 0, 4, 0), (wide, 0, 3, 1))), cotangent)
    for c in own1:
        c.wait()

    def saved(c, j):
        return [local(ab.at[i, j], dst.at[c, aligned(j * SPAN, SPAN)], asem.at[i, j]) for i, dst in enumerate((ao, bo))]

    def kept(c):
        return local(vp.at[:, aligned(c * CHUNK, CHUNK)], po.at[c], psem.at[c])

    def hidden(c):
        for n in (3, 4, 5):

            @pl.when(c + (5 - n) < chunks)
            def _(n=n):
                wide(0, n, c + (5 - n))

        due(c, ((0, (tall, 0, 1), (all_wide, 1, 0)), (1, (tall, 0, 2)), (2, (tall, 0, 3), (all_wide, 1, 1)), (3, (tall, 1, 0))))
        due(c, ((4, (tall, 0, 4), (all_wide, 1, 2)), (5, (tall, 1, 1)), (6, (tall, 1, 2), (all_wide, 1, 3))))
        cols = aligned(c * CHUNK, CHUNK)

        def span(j):
            @pl.when(c >= 1)
            def _():
                for copy in saved(c, j):
                    copy.wait()

            for u in range(UNROLL):
                r = aligned(j * SPAN + u * TILE, TILE)
                a = va[r, :]
                gate = dot(a, vg[:, :, :, cols].reshape(d, CHUNK))
                up = dot(a, vu[:, :, :, cols].reshape(d, CHUNK))
                s = 1 / (1 + jnp.exp(-gate))
                b = gate * s
                mine = pl.ds(u * TILE, TILE)
                ab[0, j, mine, :] = up * (s + b * (1 - s))
                ab[1, j, mine, :] = b
                vp[r, cols] = (b * up).astype(BF16)
            for copy in saved(c, j):
                copy.start()

        loop(spans, span)
        kept(c).start()

    loop(chunks, hidden)
    for j in range(spans):
        for copy in saved(0, j):
            copy.wait()
    tall(0, 5)
    dcopy = local(vd, wd0o, xsem.at[0])
    dcopy.start()

    def outs(b):
        s = lax.rem(b, 2)
        r = rows_of(b)
        pairs = ((th, ho.at[r]), (ta, a1.at[r]), (tt, a1t.at[:, r]))
        return [local(src.at[s], dst, sem.at[2 * i + s]) for i, (src, dst) in enumerate(pairs)]

    def down(b):
        due(b, ((1, (tall, 1, 3)), (2, (all_wide, 1, 4)), (4, (tall, 1, 4))))

        @pl.when(b >= 2)
        def _():
            for c in outs(b):
                c.wait()

        s = lax.rem(b, 2)
        r = rows_of(b)
        h = (vx[r, :].astype(F32) + rounded(dot(vp[r, :], vd[...].reshape(ff, d)))).astype(BF16)
        a = normed(h)
        th[s] = h
        ta[s] = a
        tt[s] = a.T
        for c in outs(b):
            c.start()

    loop(blocks, down)
    for b in BOTH:
        for c in outs(b):
            c.wait()
    loop(chunks, lambda c: kept(c).wait())
    dcopy.wait()
    all_wide(1, 5)
    tall(1, 5)
    for layer in BOTH:
        all_wide(layer, 6)
        tall(layer, 6)


def front(side, x, dy, wg, wu, wd):
    tokens, d = x.shape
    ff = wg.shape[2]
    chunks, dchunks = ff // CHUNK, d // CHUNK
    rows, drows = wg.shape[1], wd.shape[1]
    shape = jax.ShapeDtypeStruct
    dma = pltpu.SemaphoreType.DMA
    states, turned, wide, tall = (tokens, d), (d, tokens), (side, side, rows, ff), (side, side, drows, d)
    outs = [shape((chunks, tokens, CHUNK), F32)] * 2 + [shape((chunks, tokens, CHUNK), BF16)]
    outs += [shape(s, BF16) for s in (turned, turned, states, states, turned, tall, wide, wide, tall)]
    gathers = [dma((2, chunks, 7)), dma((2, chunks, 7)), dma((2, dchunks, 7))] * 2
    return pl.pallas_call(
        functools.partial(front_kernel, side),
        name="front",
        out_shape=outs,
        in_specs=[ANY, ANY, VMEM, VMEM, VMEM],
        out_specs=[ANY] * len(outs),
        scratch_shapes=[
            *(pltpu.VMEM(s, BF16) for s in (states, states, (tokens, ff), wide, wide, tall)),
            pltpu.VMEM((2, tokens // SPAN, SPAN, CHUNK), F32),
            *(pltpu.VMEM((2, *s), BF16) for s in ((WIDE, d), (d, WIDE), (WIDE, d), (WIDE, d))),
            dma((tokens // WIDE,)),
            dma((chunks,)),
            dma((2, tokens // SPAN)),
            dma((6,)),
            *gathers,
        ],
        compiler_params=pltpu.CompilerParams(vmem_limit_bytes=VMEM_LIMIT, collective_id=0, has_side_effects=True),
        cost_estimate=pl.CostEstimate(flops=6 * tokens * d * ff, bytes_accessed=40 * tokens * d, transcendentals=tokens * ff),
    )(x, dy, wg, wu, wd)


SUBS = ((0, 0, 0, 1), (0, 1, 0, -1), (1, 0, 1, 1), (1, 1, 1, -1))


def fetch(hidden, bufs, sems, c):
    slot = lax.rem(c, bufs.shape[0])
    return local(hidden.at[c], bufs.at[slot], sems.at[slot])


class Grads:
    def __init__(self, torus, own, dwd, wide_refs, tall_refs, gg, gu, gd, slots, stages, turn):
        self.t, self.own, self.dwd, self.out, self.gd = torus, own, dwd, (gg, gu), gd
        self.rows, self.drows = gg.shape[0], gd.shape[0]
        self.wide, self.tall = Scatter(torus, self.rows, wide_refs), Scatter(torus, self.drows, tall_refs)
        self.slots, self.stages, self.turn = slots, stages, turn

    def wide_stage(self, n, c):
        slot, stage = lax.rem(c, self.slots), lax.rem(c, self.stages)
        for sub, (which, group, axis, way) in enumerate(SUBS):
            lanes = pl.ds(group * LANES, LANES)

            def own(i, j, which=which, lanes=lanes):
                return self.own[slot, which, aligned((i * self.t.side + j) * self.rows, self.rows), lanes]

            def out(value, which=which, group=group):
                self.out[which][:, aligned(c * CHUNK + group * LANES, LANES)] = value.astype(BF16)

            self.wide.stage(n, c * len(SUBS) + sub, stage * len(SUBS) + sub, axis, way, own, out)

    def earlier(self, stages, c):
        for back, n in reversed(list(enumerate(stages, 1))):

            @pl.when(c >= back)
            def _(n=n, back=back):
                self.wide_stage(n, c - back)

    def tall_gradient(self, c, chunks, turned, hidden, bufs, sems):
        @pl.when(c + 2 < chunks)
        def _():
            fetch(hidden, bufs, sems, c + 2).start()

        fetch(hidden, bufs, sems, c).wait()
        self.dwd[aligned(c * CHUNK, CHUNK), :] = dot(turned[...], bufs[lax.rem(c, bufs.shape[0])]).T

    def tall_stage(self, n):
        for k in range(self.gd.shape[1] // LANES):
            lanes = pl.ds(k * LANES, LANES)

            def own(i, j, lanes=lanes):
                return self.dwd[aligned((i * self.t.side + j) * self.drows, self.drows), lanes]

            def out(value, lanes=lanes):
                self.gd[:, lanes] = value.astype(BF16)

            self.tall.stage(n, k, k, (k + self.turn) % 2, 1 - 2 * (k // 2 % 2), own, out)


def mid_kernel(side, slots, stages, a1, a1t, dy, dyt, h, wg, wu, wd, gg, gu, gd, dh, dht, po, dgo, duo, vg, vu, vd, vdy, own, dwd, *rest):
    wide_refs, tall_refs, (lsem, esem, wsem, ssem, psem, osem) = rest[:6], rest[6:12], rest[12:]
    t = Torus(side)
    d, ff = vg.shape
    tokens = vdy.shape[0]
    chunks = ff // CHUNK
    spans = tokens // SPAN
    grads = Grads(t, own, dwd, wide_refs, tall_refs, gg, gu, gd, slots, stages, 0)

    def first(va, vat, bufs):
        def early(j):
            r = aligned(j * SPAN, SPAN)
            return [local(s.at[r], o.at[r], esem.at[i, j]) for i, (s, o) in enumerate(((a1, va), (dy, vdy)))]

        def weights(c):
            cols = aligned(c * CHUNK, CHUNK)
            views = ((wg, vg, (slice(None), cols)), (wu, vu, (slice(None), cols)), (wd, vd, (cols,)))
            return [local(s.at[at], o.at[at], wsem.at[i, c]) for i, (s, o, at) in enumerate(views)]

        turned, last = local(a1t, vat, lsem.at[0]), local(dyt, vat, lsem.at[1])

        def begin(copies):
            for c in copies:
                c.start()

        def end(copies):
            for c in copies:
                c.wait()

        begin(weights(0))
        loop(spans, lambda j: begin(early(j)))
        t.greet(greeted(t, (1, -1)))

        def stash(c, j):
            r = aligned(j * SPAN, SPAN)
            return [local(bufs.at[i, r], o.at[c, r], ssem.at[i, j]) for i, o in enumerate((dgo, duo, po))]

        def hidden(c):
            end(weights(c))

            @pl.when(c + 1 < chunks)
            def _():
                begin(weights(c + 1))

            cols = aligned(c * CHUNK, CHUNK)

            def span(j):
                @pl.when(c == 0)
                def _():
                    end(early(j))

                @pl.when(c >= 1)
                def _():
                    end(stash(c, j))

                for u in range(UNROLL):
                    r = aligned(j * SPAN + u * TILE, TILE)
                    a = va[r, :]
                    gate = dot(a, vg[:, cols])
                    up = dot(a, vu[:, cols])
                    dp = rounded(dot_nt(vdy[r, :], vd[cols, :]))
                    s = 1 / (1 + jnp.exp(-gate))
                    b = gate * s
                    bufs[2, r, :] = (b * up).astype(BF16)
                    bufs[0, r, :] = (dp * (up * (s + b * (1 - s)))).astype(BF16)
                    bufs[1, r, :] = (dp * b).astype(BF16)
                begin(stash(c, j))

                @pl.when(jnp.logical_and(c == 0, j == 0))
                def _():
                    turned.start()

            loop(spans, span)
            slot = lax.rem(c, slots)

            @pl.when(c == 0)
            def _():
                turned.wait()

            grads.earlier((1, 3), c)
            for which in BOTH:
                own[slot, which] = dot(vat[...], bufs[which])
            grads.earlier((2, 4), c)
            grads.wide_stage(0, c)

        loop(chunks, hidden)
        last.start()
        for j in range(spans):
            end(stash(0, j))

        for c in range(2):
            fetch(po, bufs, psem, c).start()
        last.wait()

        def gradient(c):
            grads.tall_gradient(c, chunks, vat, po, bufs, psem)
            for at, n, back in ((0, 3, 2), (0, 1, 1), (1, 4, 2), (2, 2, 1), (4, 3, 1), (6, 4, 1)):

                @pl.when(c == at)
                def _(n=n, back=back):
                    grads.wide_stage(n, chunks - back)

        loop(chunks, gradient)
        grads.tall_stage(0)

    pl.run_scoped(
        first,
        *(pltpu.VMEM(s, BF16) for s in ((tokens, d), (d, tokens), (3, tokens, CHUNK))),
    )

    def second(tg, tu, th, to, tt):
        blocks = tokens // WIDE

        def ins(b, s):
            r = aligned(b * WIDE, WIDE)
            return [local(src, dst.at[s], osem.at[i, s]) for i, (src, dst) in enumerate(((dgo.at[:, r], tg), (duo.at[:, r], tu), (h.at[r], th)))]

        def outs(b, s):
            r = aligned(b * WIDE, WIDE)
            return [local(src.at[s], dst, osem.at[3 + i, s]) for i, (src, dst) in enumerate(((to, dh.at[r]), (tt, dht.at[:, r])))]

        for c in ins(0, 0):
            c.start()

        def block(b):
            s = lax.rem(b, 2)

            @pl.when(b + 1 < blocks)
            def _():
                for c in ins(b + 1, 1 - s):
                    c.start()

            for at, n in ((3, 1), (5, 2), (6, 3), (7, 4)):

                @pl.when(b == at)
                def _(n=n):
                    grads.tall_stage(n)

            for c in ins(b, s):
                c.wait()

            @pl.when(b >= 2)
            def _():
                for c in outs(b - 2, s):
                    c.wait()

            r = aligned(b * WIDE, WIDE)
            sides = [jnp.concatenate([half[s, c] for c in range(chunks)], axis=1) for half in (tg, tu)]
            da = rounded(rounded(dot_nt(sides[0], vg[...])) + rounded(dot_nt(sides[1], vu[...])))
            wide = th[s].astype(F32)
            scale = scale_of(wide)
            across = jnp.sum(da * wide, -1, keepdims=True)
            dn = da * scale - wide * (across * (scale * scale * scale) / d)
            value = (vdy[r, :].astype(F32) + rounded(dn)).astype(BF16)
            to[s] = value
            tt[s] = value.T
            for c in outs(b, s):
                c.start()

        loop(blocks, block)
        for s in BOTH:
            for c in outs(s, s):
                c.wait()

    pl.run_scoped(
        second,
        *(pltpu.VMEM((2, *s), BF16) for s in ((chunks, WIDE, CHUNK), (chunks, WIDE, CHUNK), (WIDE, d), (WIDE, d), (d, WIDE))),
    )


def mid(side, rows, drows, a1, a1t, dy, dyt, h, wg, wu, wd):
    tokens, d = a1.shape
    ff = wg.shape[1]
    chunks = ff // CHUNK
    slots, stages = 2, 3
    shape = jax.ShapeDtypeStruct
    dma = pltpu.SemaphoreType.DMA
    return pl.pallas_call(
        functools.partial(mid_kernel, side, slots, stages),
        name="mid",
        out_shape=[shape(s, BF16) for s in ((rows, ff), (rows, ff), (drows, d), (tokens, d), (d, tokens), *[(chunks, tokens, CHUNK)] * 3)],
        in_specs=[ANY] * 8,
        out_specs=[VMEM] * 3 + [ANY] * 5,
        scratch_shapes=[
            *(pltpu.VMEM(s, BF16) for s in ((d, ff), (d, ff), (ff, d), (tokens, d))),
            pltpu.VMEM((slots, 2, d, CHUNK), F32),
            pltpu.VMEM((ff, d), F32),
            *Scatter.scratch(side, rows, chunks * len(SUBS), stages * len(SUBS)),
            *Scatter.scratch(side, drows, d // LANES, d // LANES),
            *(dma(s) for s in ((2,), (2, tokens // SPAN), (3, chunks), (3, tokens // SPAN), (3,), (5, 2))),
        ],
        compiler_params=pltpu.CompilerParams(vmem_limit_bytes=VMEM_LIMIT, collective_id=1, has_side_effects=True),
        cost_estimate=pl.CostEstimate(flops=16 * tokens * d * ff, bytes_accessed=40 * tokens * d, transcendentals=tokens * ff),
    )(a1, a1t, dy, dyt, h, wg, wu, wd)


def back_kernel(side, slots, stages, dh, dht, a0t, po, ao, bo, wd, g1, u1, d1, gg, gu, gd, total, vd, vdh, vdht, vat, pair, ab, own, dwd, *rest):
    wide_refs, tall_refs, (tiles, lsem, asem, psem, tsem) = rest[:6], rest[6:12], rest[12:]
    t = Torus(side)
    tokens, d = vdh.shape
    ff = vd.shape[0]
    chunks, spans = ff // CHUNK, tokens // SPAN
    depth = ab.shape[1]
    grads = Grads(t, own, dwd, wide_refs, tall_refs, gg, gu, gd, slots, stages, 1)

    def saved(step):
        c, j, slot = step // spans, lax.rem(step, spans), lax.rem(step, depth)
        return [local(s.at[c, aligned(j * SPAN, SPAN)], ab.at[i, slot], asem.at[i, slot]) for i, s in enumerate((ao, bo))]

    def begin(copies):
        for c in copies:
            c.start()

    def end(copies):
        for c in copies:
            c.wait()

    ins = [local(s, o, lsem.at[i]) for i, (s, o) in enumerate(((dht, vdht), (dh, vdh), (a0t, vat), (wd, vd)))]
    ins[0].start()
    for c in range(2):
        fetch(po, pair, psem, c).start()
    t.greet(greeted(t, range(1, side)))
    ins[0].wait()

    def gradient(c):
        @pl.when(c == 1)
        def _():
            begin(ins[1:])

        for step in range(depth - 1):

            @pl.when(c == 2 + step)
            def _(step=step):
                begin(saved(step))

        grads.tall_gradient(c, chunks, vdht, po, pair, psem)

    loop(chunks, gradient)
    grads.tall_stage(0)
    end(ins[1:])

    def hidden(c):
        cols = aligned(c * CHUNK, CHUNK)

        def span(j):
            step = c * spans + j

            @pl.when(step + depth - 1 < chunks * spans)
            def _():
                begin(saved(step + depth - 1))

            end(saved(step))
            slot = lax.rem(step, depth)
            for u in range(UNROLL):
                r = aligned(j * SPAN + u * TILE, TILE)
                mine = pl.ds(u * TILE, TILE)
                dp = rounded(dot_nt(vdh[r, :], vd[cols, :]))
                for i in BOTH:
                    pair[i, r, :] = (dp * ab[i, slot, mine, :]).astype(BF16)

        loop(spans, span)

        for n in (1, 2, 3, 4):

            @pl.when(c == n + 1)
            def _(n=n):
                grads.tall_stage(n)

        slot = lax.rem(c, slots)
        for which in BOTH:
            own[slot, which] = dot(vat[...], pair[which])
        grads.earlier((1, 2, 3, 4), c)
        grads.wide_stage(0, c)

    loop(chunks, hidden)
    for first in (1, 2, 3, 4):
        for back, n in enumerate(range(first, 5), 1):
            grads.wide_stage(n, chunks - back)

    squares = functools.reduce(lambda a, b: a + b, [jnp.sum(jnp.square(g[...].astype(F32))) for g in (g1, u1, d1, gg, gu, gd)])
    value = jnp.full(total.shape, squares, F32)
    for axis in BOTH:
        tiles[axis, 0] = value
        sent = [remote(tiles.at[axis, 0], tiles.at[axis, away], tsem.at[axis, 0, away], tsem.at[axis, 1, away], t.id(axis, away)) for away in range(1, side)]
        begin(sent)
        end(sent)
        value = functools.reduce(lambda a, b: a + b, [tiles[axis, i] for i in range(side)])
    total[...] = value


def back(side, dh, dht, a0t, po, ao, bo, wd, g1, u1, d1):
    tokens, d = dh.shape
    ff = wd.shape[0]
    rows, drows = g1.shape[0], d1.shape[0]
    chunks = ff // CHUNK
    slots, stages, depth = 3, 4, 5
    shape = jax.ShapeDtypeStruct
    dma = pltpu.SemaphoreType.DMA
    return pl.pallas_call(
        functools.partial(back_kernel, side, slots, stages),
        name="back",
        out_shape=[shape((rows, ff), BF16), shape((rows, ff), BF16), shape((drows, d), BF16), shape((8, LANES), F32)],
        in_specs=[ANY] * 7 + [VMEM] * 3,
        out_specs=[VMEM] * 4,
        scratch_shapes=[
            *(pltpu.VMEM(s, BF16) for s in ((ff, d), (tokens, d), (d, tokens), (d, tokens), (3, tokens, CHUNK))),
            pltpu.VMEM((2, depth, SPAN, CHUNK), F32),
            pltpu.VMEM((slots, 2, d, CHUNK), F32),
            pltpu.VMEM((ff, d), F32),
            *Scatter.scratch(side, rows, chunks * len(SUBS), stages * len(SUBS)),
            *Scatter.scratch(side, drows, d // LANES, d // LANES),
            pltpu.VMEM((2, side, 8, LANES), F32),
            *(dma(s) for s in ((4,), (2, depth), (3,), (2, 2, side))),
        ],
        compiler_params=pltpu.CompilerParams(vmem_limit_bytes=VMEM_LIMIT, collective_id=2, has_side_effects=True),
        cost_estimate=pl.CostEstimate(flops=8 * tokens * d * ff, bytes_accessed=40 * tokens * d, transcendentals=0),
    )(dh, dht, a0t, po, ao, bo, wd, g1, u1, d1)


def adamw(w, m, v, g):
    m = 0.9 * m + 0.1 * g
    v = 0.95 * v + 0.05 * g * g
    step = m * lax.rsqrt(v + 1e-8) + 0.1 * w
    return (w - 0.02 * step).astype(BF16), m, v


def solution(mesh):
    side = math.isqrt(mesh.shape["dp"])
    group = side * side

    def step(x, dy, *arrays):
        weights, m, v = (arrays[i : i + 3] for i in (0, 3, 6))
        wg, wu, wd = weights
        x, dy = x[0], dy[0]
        d, ff = x.shape[1], wg.shape[2]
        ao, bo, po, a0t, dyt, h, a1, a1t, wd0, wg1, wu1, wd1 = front(side, x, dy, wg, wu, wd)
        last = mid(side, wg.shape[1], wd.shape[1], a1, a1t, dy, dyt, h, wg1.reshape(d, ff), wu1.reshape(d, ff), wd1.reshape(ff, d))
        g1, dh, dht = last[:3], last[3], last[4]
        *g0, total = back(side, dh, dht, a0t, po, ao, bo, wd0.reshape(ff, d), *g1)
        count = group * sum(g.size for g in (*g0, *g1))
        factor = jnp.minimum(1.0, 0.5 * lax.rsqrt(total[0, 0] / count + 1e-30))
        new = [
            adamw(w.astype(F32), m, v, jnp.stack([first, second]).astype(F32) * factor)
            for w, m, v, first, second in zip(weights, m, v, g0, g1, strict=True)
        ]
        return tuple(one[which] for which in range(3) for one in new)

    states, cut = P(("rep", "dp"), None, None), P(None, "dp", None)
    return jax.shard_map(
        step,
        mesh=mesh,
        in_specs=(states, states) + (cut,) * 9,
        out_specs=(P("rep", "dp", None),) * 9,
        check_vma=False,
    )
```

```python
import functools
import math

import jax
import jax.numpy as jnp
from jax import lax
from jax.experimental import pallas as pl
from jax.experimental.pallas import tpu as pltpu
from jax.sharding import PartitionSpec as P

BF16, F32 = jnp.bfloat16, jnp.float32
LANES = 128
CHUNK = 2 * LANES
TILE = 256
UNROLL = 4
SPAN = TILE * UNROLL
WIDE = 512
EPS = 1e-6
BOTH = (0, 1)
ANY = pl.BlockSpec(memory_space=pl.ANY)
VMEM = pl.BlockSpec(memory_space=pltpu.VMEM)
MESH_IDS = pl.DeviceIdType.MESH
VMEM_LIMIT = 67_000_000


def dot(a, b):
    return jnp.dot(a, b, preferred_element_type=F32)


def dot_nt(a, b):
    return lax.dot_general(a, b, (((1,), (1,)), ((), ())), preferred_element_type=F32)


def rounded(x):
    return x.astype(BF16).astype(F32)


def aligned(start, size):
    return pl.ds(pl.multiple_of(start, size), size)


def local(src, dst, sem):
    return pltpu.make_async_copy(src, dst, sem)


def loop(n, body):
    def step(i, carry):
        body(i)
        return carry

    lax.fori_loop(0, n, step, 0)


class Torus:
    def __init__(self, side):
        index = lax.axis_index("dp")
        self.side = side
        self.at = (index // side, lax.rem(index, side))

    def near(self, axis, away):
        return lax.rem(self.at[axis] + away + self.side, self.side)

    def id(self, axis, away):
        place = [self.at[0], self.at[1]]
        place[axis] = self.near(axis, away)
        return {"dp": place[0] * self.side + place[1]}

    def partner(self):
        rep = lax.axis_index("rep")
        return {"rep": rep + 1 - 2 * lax.rem(rep, 2)}

    def greet(self, targets):
        barrier = pltpu.get_barrier_semaphore()
        for target in targets:
            pl.semaphore_signal(barrier, inc=1, device_id=target, device_id_type=MESH_IDS)
        pl.semaphore_wait(barrier, len(targets))


def remote(src, dst, send, recv, target):
    return pltpu.make_async_remote_copy(src_ref=src, dst_ref=dst, send_sem=send, recv_sem=recv, device_id=target, device_id_type=MESH_IDS)


class Gather:
    def __init__(self, torus, full, own, sems):
        self.t, self.full, self.own, self.send, self.recv = torus, full, own, sems.at[0], sems.at[1]
        self.core = lax.rem(lax.axis_index("rep"), 2)

    def cols(self, piece):
        return aligned(piece * CHUNK + self.core * LANES, LANES)

    def copy(self, k, which, src, dst, target):
        return remote(src, dst, self.send.at[k, which], self.recv.at[k, which], target)

    def block(self, axis, along, piece):
        i = (along, self.t.at[1]) if axis == 0 else (self.t.at[0], along)
        return self.full.at[i[0], i[1], :, self.cols(piece)]

    def line(self, axis, across, piece):
        c = self.cols(piece)
        return self.full.at[:, across, :, c] if axis == 0 else self.full.at[across, :, :, c]

    def near_pair(self, k, piece, axis):
        b = self.block(axis, self.t.at[axis], piece)
        own = self.own.at[:, self.cols(piece)]
        return [self.copy(k, n, own, b, self.t.id(axis, 1 - 2 * n)) for n in BOTH]

    def far_block(self, k, piece, axis, odd):
        b = self.block(axis, self.t.near(axis, 2 * odd - 1), piece)
        return self.copy(k, 2, b, b, self.t.id(axis, 1 - 2 * odd))

    def line_pair(self, k, piece, axis):
        mine = self.line(axis, self.t.at[1 - axis], piece)
        return [self.copy(k, 3 + n, mine, mine, self.t.id(1 - axis, 1 - 2 * n)) for n in BOTH]

    def far_line(self, k, piece, axis, odd):
        line = self.line(axis, self.t.near(1 - axis, 2 * odd - 1), piece)
        return self.copy(k, 5, line, line, self.t.id(1 - axis, 1 - 2 * odd))

    def across(self, k, piece):
        whole = self.full.at[:, :, :, self.cols(piece)]
        return self.copy(k, 6, whole, whole, self.t.partner())

    def wait(self, k, which, like):
        self.copy(k, which, like, like, self.t.partner()).wait_recv()

    def stage(self, n, k, piece, axis, odd):
        block = self.block(axis, self.t.at[axis], piece)
        line = self.line(axis, self.t.at[1 - axis], piece)
        if n == 0:
            for c in self.near_pair(k, piece, axis):
                c.start()
        elif n == 1:
            self.wait(k, odd, block)
            self.far_block(k, piece, axis, odd).start()
        elif n == 2:
            self.wait(k, 1 - odd, block)
            self.wait(k, 2, block)
            for c in self.line_pair(k, piece, axis):
                c.start()
        elif n == 3:
            self.wait(k, 3 + odd, line)
            self.far_line(k, piece, axis, odd).start()
        elif n == 4:
            self.wait(k, 4 - odd, line)
            self.wait(k, 5, line)
            self.across(k, piece).start()
        elif n == 5:
            self.wait(k, 6, self.full.at[:, :, :, self.cols(piece)])
        else:
            for c in self.near_pair(k, piece, axis) + self.line_pair(k, piece, axis):
                c.wait_send()
            self.far_block(k, piece, axis, odd).wait_send()
            self.far_line(k, piece, axis, odd).wait_send()
            self.across(k, piece).wait_send()


class Scatter:
    def __init__(self, torus, rows, refs):
        self.t, self.rows = torus, rows
        self.sa, self.ra, self.sb, self.rb, self.q, self.sems = refs

    @staticmethod
    def scratch(side, rows, pieces, slots):
        return [
            pltpu.VMEM((slots, 3, side, rows, LANES), BF16),
            pltpu.VMEM((pieces, 3, side, rows, LANES), BF16),
            pltpu.VMEM((slots, 3, rows, LANES), BF16),
            pltpu.VMEM((pieces, 3, rows, LANES), BF16),
            pltpu.VMEM((slots, side, rows, LANES), F32),
            pltpu.SemaphoreType.DMA((pieces, 2, 2, 3)),
        ]

    def copy(self, phase, k, slot, which, axis, way):
        src, dst = ((self.sa, self.ra), (self.sb, self.rb))[phase]
        if phase:
            axis = 1 - axis
        target = self.t.id(axis, -way if which == 1 else way)
        sems = self.sems.at[k, phase]
        return remote(src.at[slot, which], dst.at[k, which], sems.at[0, which], sems.at[1, which], target)

    def stage(self, n, k, slot, axis, way, own, out):
        t, side, other = self.t, self.t.side, 1 - axis

        def term(along, across):
            return own(along, across) if axis == 0 else own(across, along)

        if n == 0:
            for which, away in ((0, 2), (1, -way)):
                for i in range(side):
                    self.sa[slot, which, i] = term(t.near(axis, away), i).astype(BF16)
                self.copy(0, k, slot, which, axis, way).start()
        elif n == 1:
            self.copy(0, k, slot, 0, axis, way).wait_recv()
            for i in range(side):
                self.sa[slot, 2, i] = (term(t.near(axis, way), i) + self.ra[k, 0, i].astype(F32)).astype(BF16)
            self.copy(0, k, slot, 2, axis, way).start()
        elif n == 2:
            for which in (1, 2):
                self.copy(0, k, slot, which, axis, way).wait_recv()
            for i in range(side):
                self.q[slot, i] = term(t.at[axis], i) + self.ra[k, 1, i].astype(F32) + self.ra[k, 2, i].astype(F32)
            for which, away in ((0, 2), (1, -way)):
                self.sb[slot, which] = self.q[slot, t.near(other, away)].astype(BF16)
                self.copy(1, k, slot, which, axis, way).start()
        elif n == 3:
            self.copy(1, k, slot, 0, axis, way).wait_recv()
            self.sb[slot, 2] = (self.q[slot, t.near(other, way)] + self.rb[k, 0].astype(F32)).astype(BF16)
            self.copy(1, k, slot, 2, axis, way).start()
        else:
            for which in (1, 2):
                self.copy(1, k, slot, which, axis, way).wait_recv()
            out(self.q[slot, t.at[other]] + self.rb[k, 1].astype(F32) + self.rb[k, 2].astype(F32))
            for phase in BOTH:
                for which in range(3):
                    self.copy(phase, k, slot, which, axis, way).wait_send()


def greeted(t, aways):
    return [t.id(axis, away) for axis in BOTH for away in aways]


def scale_of(wide):
    return lax.rsqrt(jnp.mean(wide * wide, -1, keepdims=True) + EPS)


def normed(h):
    wide = h.astype(F32)
    return (wide * scale_of(wide)).astype(BF16)


def front_kernel(side, x, dy, wg, wu, wd, ao, bo, po, a0t, dyt, ho, a1, a1t, wd0o, wg1, wu1, wd1, vx, va, vp, vg, vu, vd, ab, td, tt, th, ta, xsem, psem, asem, sem, *gather_sems):
    t = Torus(side)
    tokens, ff = vp.shape
    d = vx.shape[1]
    chunks, dchunks, blocks, spans = ff // CHUNK, d // CHUNK, tokens // WIDE, tokens // SPAN
    me = t.at

    def rows_of(b):
        return aligned(b * WIDE, WIDE)

    def xin(b):
        return local(x.at[rows_of(b)], vx.at[rows_of(b)], xsem.at[b])

    loop(blocks, lambda b: xin(b).start())
    for full, shard in ((vg, wg), (vu, wu), (vd, wd)):
        full[me[0], me[1]] = shard[0]
    own1 = [local(s.at[1], o.at[me[0], me[1]], psem.at[i]) for i, (s, o) in enumerate(((wg, wg1), (wu, wu1), (wd, wd1)))]
    for c in own1:
        c.start()
    t.greet([*greeted(t, (1, -1)), t.partner()])

    shards, layers = (wg, wu, wd), ((vg, vu, vd), (wg1, wu1, wd1))
    gathers = [[Gather(t, f, s.at[n], gather_sems[3 * n + i]) for i, (f, s) in enumerate(zip(fulls, shards))] for n, fulls in enumerate(layers)]

    def wide(layer, n, c):
        for axis in BOTH:
            gathers[layer][axis].stage(n, c, c, axis, lax.rem(c, 2))

    def tall(layer, n):
        for c in range(dchunks):
            gathers[layer][2].stage(n, c, c, (c + layer) % 2, (c // 2 + layer) % 2)

    def all_wide(layer, n):
        loop(chunks, lambda c: wide(layer, n, c))

    def due(i, plan):
        for at, *work in plan:

            @pl.when(i == at)
            def _(work=work):
                for f, *args in work:
                    f(*args)

    all_wide(0, 0)

    def turned(dst, b):
        slot = lax.rem(b, 2)
        return local(tt.at[slot], dst.at[:, rows_of(b)], sem.at[slot])

    def turn(dst, plan, get):
        def block(b):
            @pl.when(b >= 2)
            def _():
                turned(dst, b).wait()

            for q in range(0, WIDE, LANES):
                tt[lax.rem(b, 2), :, pl.ds(q, LANES)] = get(b, q).T
            turned(dst, b).start()
            due(b, plan)

        loop(blocks, block)
        for b in BOTH:
            turned(dst, b).wait()

    def first_states(b, q):
        if q == 0:
            xin(b).wait()
        r = aligned(b * WIDE + q, LANES)
        a = normed(vx[r, :])
        va[r, :] = a
        return a

    def dyin(b):
        slot = lax.rem(b, 2)
        return local(dy.at[rows_of(b)], td.at[slot], sem.at[2 + slot])

    def cotangent(b, q):
        if q == 0:

            @pl.when(b + 1 < blocks)
            def _():
                dyin(b + 1).start()

            dyin(b).wait()
        return td[lax.rem(b, 2), pl.ds(q, LANES), :]

    dyin(0).start()
    turn(a0t, ((2, (all_wide, 0, 1)), (6, (all_wide, 0, 2), (tall, 0, 0))), first_states)
    turn(dyt, ((2, (wide, 0, 3, 0)), (6, (wide, 0, 4, 0), (wide, 0, 3, 1))), cotangent)
    for c in own1:
        c.wait()

    def saved(c, j):
        return [local(ab.at[i, j], dst.at[c, aligned(j * SPAN, SPAN)], asem.at[i, j]) for i, dst in enumerate((ao, bo))]

    def kept(c):
        return local(vp.at[:, aligned(c * CHUNK, CHUNK)], po.at[c], psem.at[c])

    def hidden(c):
        wide(0, 5, c)
        due(c, ((0, (tall, 0, 1), (all_wide, 1, 0)), (1, (tall, 0, 2)), (2, (tall, 0, 3), (all_wide, 1, 1)), (3, (tall, 1, 0))))
        due(c, ((4, (tall, 0, 4), (all_wide, 1, 2)), (5, (tall, 1, 1)), (6, (tall, 1, 2), (all_wide, 1, 3))))
        cols = aligned(c * CHUNK, CHUNK)

        def span(j):
            @pl.when(c >= 1)
            def _():
                for copy in saved(c, j):
                    copy.wait()

            for u in range(UNROLL):
                r = aligned(j * SPAN + u * TILE, TILE)
                a = va[r, :]
                gate = dot(a, vg[:, :, :, cols].reshape(d, CHUNK))
                up = dot(a, vu[:, :, :, cols].reshape(d, CHUNK))
                s = 1 / (1 + jnp.exp(-gate))
                b = gate * s
                mine = pl.ds(u * TILE, TILE)
                ab[0, j, mine, :] = up * (s + b * (1 - s))
                ab[1, j, mine, :] = b
                vp[r, cols] = (b * up).astype(BF16)
            for copy in saved(c, j):
                copy.start()

            for ahead, n in ((1, 4), (2, 3)):

                @pl.when(jnp.logical_and(j == ahead, c + ahead < chunks))
                def _(ahead=ahead, n=n):
                    wide(0, n, c + ahead)

        loop(spans, span)
        kept(c).start()

    loop(chunks, hidden)
    for j in range(spans):
        for copy in saved(0, j):
            copy.wait()
    tall(0, 5)
    dcopy = local(vd, wd0o, xsem.at[0])
    dcopy.start()

    def outs(b):
        s = lax.rem(b, 2)
        r = rows_of(b)
        pairs = ((th, ho.at[r]), (ta, a1.at[r]), (tt, a1t.at[:, r]))
        return [local(src.at[s], dst, sem.at[2 * i + s]) for i, (src, dst) in enumerate(pairs)]

    def down(b):
        due(b, ((1, (tall, 1, 3)), (2, (all_wide, 1, 4)), (4, (tall, 1, 4))))

        @pl.when(b >= 2)
        def _():
            for c in outs(b):
                c.wait()

        s = lax.rem(b, 2)
        r = rows_of(b)
        h = (vx[r, :].astype(F32) + rounded(dot(vp[r, :], vd[...].reshape(ff, d)))).astype(BF16)
        a = normed(h)
        th[s] = h
        ta[s] = a
        tt[s] = a.T
        for c in outs(b):
            c.start()

    loop(blocks, down)
    for b in BOTH:
        for c in outs(b):
            c.wait()
    loop(chunks, lambda c: kept(c).wait())
    dcopy.wait()
    all_wide(1, 5)
    tall(1, 5)
    for layer in BOTH:
        all_wide(layer, 6)
        tall(layer, 6)


def front(side, x, dy, wg, wu, wd):
    tokens, d = x.shape
    ff = wg.shape[2]
    chunks, dchunks = ff // CHUNK, d // CHUNK
    rows, drows = wg.shape[1], wd.shape[1]
    shape = jax.ShapeDtypeStruct
    dma = pltpu.SemaphoreType.DMA
    states, turned, wide, tall = (tokens, d), (d, tokens), (side, side, rows, ff), (side, side, drows, d)
    outs = [shape((chunks, tokens, CHUNK), F32)] * 2 + [shape((chunks, tokens, CHUNK), BF16)]
    outs += [shape(s, BF16) for s in (turned, turned, states, states, turned, tall, wide, wide, tall)]
    gathers = [dma((2, chunks, 7)), dma((2, chunks, 7)), dma((2, dchunks, 7))] * 2
    return pl.pallas_call(
        functools.partial(front_kernel, side),
        name="front",
        out_shape=outs,
        in_specs=[ANY, ANY, VMEM, VMEM, VMEM],
        out_specs=[ANY] * len(outs),
        scratch_shapes=[
            *(pltpu.VMEM(s, BF16) for s in (states, states, (tokens, ff), wide, wide, tall)),
            pltpu.VMEM((2, tokens // SPAN, SPAN, CHUNK), F32),
            *(pltpu.VMEM((2, *s), BF16) for s in ((WIDE, d), (d, WIDE), (WIDE, d), (WIDE, d))),
            dma((tokens // WIDE,)),
            dma((chunks,)),
            dma((2, tokens // SPAN)),
            dma((6,)),
            *gathers,
        ],
        compiler_params=pltpu.CompilerParams(vmem_limit_bytes=VMEM_LIMIT, collective_id=0, has_side_effects=True),
        cost_estimate=pl.CostEstimate(flops=6 * tokens * d * ff, bytes_accessed=40 * tokens * d, transcendentals=tokens * ff),
    )(x, dy, wg, wu, wd)


SUBS = ((0, 0, 0, 1), (0, 1, 0, -1), (1, 0, 1, 1), (1, 1, 1, -1))


def fetch(hidden, bufs, sems, c):
    slot = lax.rem(c, bufs.shape[0])
    return local(hidden.at[c], bufs.at[slot], sems.at[slot])


class Grads:
    def __init__(self, torus, own, dwd, wide_refs, tall_refs, gg, gu, gd, slots, stages, turn):
        self.t, self.own, self.dwd, self.out, self.gd = torus, own, dwd, (gg, gu), gd
        self.rows, self.drows = gg.shape[0], gd.shape[0]
        self.wide, self.tall = Scatter(torus, self.rows, wide_refs), Scatter(torus, self.drows, tall_refs)
        self.slots, self.stages, self.turn = slots, stages, turn

    def wide_stage(self, n, c):
        slot, stage = lax.rem(c, self.slots), lax.rem(c, self.stages)
        for sub, (which, group, axis, way) in enumerate(SUBS):
            lanes = pl.ds(group * LANES, LANES)

            def own(i, j, which=which, lanes=lanes):
                return self.own[slot, which, aligned((i * self.t.side + j) * self.rows, self.rows), lanes]

            def out(value, which=which, group=group):
                self.out[which][:, aligned(c * CHUNK + group * LANES, LANES)] = value.astype(BF16)

            self.wide.stage(n, c * len(SUBS) + sub, stage * len(SUBS) + sub, axis, way, own, out)

    def earlier(self, stages, c):
        for back, n in reversed(list(enumerate(stages, 1))):

            @pl.when(c >= back)
            def _(n=n, back=back):
                self.wide_stage(n, c - back)

    def tall_gradient(self, c, chunks, turned, hidden, bufs, sems):
        @pl.when(c + 2 < chunks)
        def _():
            fetch(hidden, bufs, sems, c + 2).start()

        fetch(hidden, bufs, sems, c).wait()
        self.dwd[aligned(c * CHUNK, CHUNK), :] = dot(turned[...], bufs[lax.rem(c, bufs.shape[0])]).T

    def tall_pairs(self, i, starts, waits):
        for pair in range(starts):
            for n, wait in enumerate(waits):

                @pl.when(i == pair + wait)
                def _(n=n, pair=pair):
                    self.tall_stage(n, pair)

    def tall_stage(self, n, pair):
        for k in (2 * pair, 2 * pair + 1):
            lanes = pl.ds(k * LANES, LANES)

            def own(i, j, lanes=lanes):
                return self.dwd[aligned((i * self.t.side + j) * self.drows, self.drows), lanes]

            def out(value, lanes=lanes):
                self.gd[:, lanes] = value.astype(BF16)

            self.tall.stage(n, k, k, (k + self.turn) % 2, 1 - 2 * (k // 2 % 2), own, out)


def mid_kernel(side, slots, stages, a1, a1t, dy, dyt, h, wg, wu, wd, gg, gu, gd, dh, dht, po, dgo, duo, vg, vu, vd, vdy, own, dwd, *rest):
    wide_refs, tall_refs, (lsem, esem, wsem, ssem, psem, osem) = rest[:6], rest[6:12], rest[12:]
    t = Torus(side)
    d, ff = vg.shape
    tokens = vdy.shape[0]
    chunks = ff // CHUNK
    spans = tokens // SPAN
    grads = Grads(t, own, dwd, wide_refs, tall_refs, gg, gu, gd, slots, stages, 0)

    def first(va, vat, bufs):
        def early(j):
            r = aligned(j * SPAN, SPAN)
            return [local(s.at[r], o.at[r], esem.at[i, j]) for i, (s, o) in enumerate(((a1, va), (dy, vdy)))]

        def weights(c):
            cols = aligned(c * CHUNK, CHUNK)
            views = ((wg, vg, (slice(None), cols)), (wu, vu, (slice(None), cols)), (wd, vd, (cols,)))
            return [local(s.at[at], o.at[at], wsem.at[i, c]) for i, (s, o, at) in enumerate(views)]

        turned, last = local(a1t, vat, lsem.at[0]), local(dyt, vat, lsem.at[1])

        def begin(copies):
            for c in copies:
                c.start()

        def end(copies):
            for c in copies:
                c.wait()

        begin(weights(0))
        loop(spans, lambda j: begin(early(j)))
        t.greet(greeted(t, (1, -1)))

        def stash(c, j):
            r = aligned(j * SPAN, SPAN)
            return [local(bufs.at[i, r], o.at[c, r], ssem.at[i, j]) for i, o in enumerate((dgo, duo, po))]

        def hidden(c):
            end(weights(c))

            @pl.when(c + 1 < chunks)
            def _():
                begin(weights(c + 1))

            cols = aligned(c * CHUNK, CHUNK)

            def span(j):
                @pl.when(c == 0)
                def _():
                    end(early(j))

                @pl.when(c >= 1)
                def _():
                    end(stash(c, j))

                for u in range(UNROLL):
                    r = aligned(j * SPAN + u * TILE, TILE)
                    a = va[r, :]
                    gate = dot(a, vg[:, cols])
                    up = dot(a, vu[:, cols])
                    dp = rounded(dot_nt(vdy[r, :], vd[cols, :]))
                    s = 1 / (1 + jnp.exp(-gate))
                    b = gate * s
                    bufs[2, r, :] = (b * up).astype(BF16)
                    bufs[0, r, :] = (dp * (up * (s + b * (1 - s)))).astype(BF16)
                    bufs[1, r, :] = (dp * b).astype(BF16)
                begin(stash(c, j))

                @pl.when(jnp.logical_and(c == 0, j == 0))
                def _():
                    turned.start()

            loop(spans, span)
            slot = lax.rem(c, slots)

            @pl.when(c == 0)
            def _():
                turned.wait()

            grads.earlier((1, 3), c)
            for which in BOTH:
                own[slot, which] = dot(vat[...], bufs[which])
            grads.earlier((2, 4), c)
            grads.wide_stage(0, c)

        loop(chunks, hidden)
        last.start()
        for j in range(spans):
            end(stash(0, j))

        for c in range(2):
            fetch(po, bufs, psem, c).start()
        last.wait()

        def gradient(c):
            grads.tall_gradient(c, chunks, vat, po, bufs, psem)
            for at, n, back in ((0, 3, 2), (0, 1, 1), (1, 4, 2), (2, 2, 1), (4, 3, 1), (6, 4, 1)):

                @pl.when(c == at)
                def _(n=n, back=back):
                    grads.wide_stage(n, chunks - back)

        loop(chunks, gradient)

    pl.run_scoped(
        first,
        *(pltpu.VMEM(s, BF16) for s in ((tokens, d), (d, tokens), (3, tokens, CHUNK))),
    )

    def second(tg, tu, th, to, tt):
        blocks = tokens // WIDE
        pairs, waits = d // CHUNK, (0, 2, 4, 5, 6)

        def ins(b, s):
            r = aligned(b * WIDE, WIDE)
            return [local(src, dst.at[s], osem.at[i, s]) for i, (src, dst) in enumerate(((dgo.at[:, r], tg), (duo.at[:, r], tu), (h.at[r], th)))]

        def outs(b, s):
            r = aligned(b * WIDE, WIDE)
            return [local(src.at[s], dst, osem.at[3 + i, s]) for i, (src, dst) in enumerate(((to, dh.at[r]), (tt, dht.at[:, r])))]

        for c in ins(0, 0):
            c.start()

        def block(b):
            s = lax.rem(b, 2)

            @pl.when(b + 1 < blocks)
            def _():
                for c in ins(b + 1, 1 - s):
                    c.start()

            grads.tall_pairs(b, pairs, waits)

            for c in ins(b, s):
                c.wait()

            @pl.when(b >= 2)
            def _():
                for c in outs(b - 2, s):
                    c.wait()

            r = aligned(b * WIDE, WIDE)
            sides = [jnp.concatenate([half[s, c] for c in range(chunks)], axis=1) for half in (tg, tu)]
            da = rounded(rounded(dot_nt(sides[0], vg[...])) + rounded(dot_nt(sides[1], vu[...])))
            wide = th[s].astype(F32)
            scale = scale_of(wide)
            across = jnp.sum(da * wide, -1, keepdims=True)
            dn = da * scale - wide * (across * (scale * scale * scale) / d)
            value = (vdy[r, :].astype(F32) + rounded(dn)).astype(BF16)
            to[s] = value
            tt[s] = value.T
            for c in outs(b, s):
                c.start()

        loop(blocks, block)
        for i in range(blocks, pairs + waits[-1]):
            for pair in range(pairs):
                for n, wait in enumerate(waits):
                    if i == pair + wait:
                        grads.tall_stage(n, pair)
        for s in BOTH:
            for c in outs(s, s):
                c.wait()

    pl.run_scoped(
        second,
        *(pltpu.VMEM((2, *s), BF16) for s in ((chunks, WIDE, CHUNK), (chunks, WIDE, CHUNK), (WIDE, d), (WIDE, d), (d, WIDE))),
    )


def mid(side, rows, drows, a1, a1t, dy, dyt, h, wg, wu, wd):
    tokens, d = a1.shape
    ff = wg.shape[1]
    chunks = ff // CHUNK
    slots, stages = 2, 3
    shape = jax.ShapeDtypeStruct
    dma = pltpu.SemaphoreType.DMA
    return pl.pallas_call(
        functools.partial(mid_kernel, side, slots, stages),
        name="mid",
        out_shape=[shape(s, BF16) for s in ((rows, ff), (rows, ff), (drows, d), (tokens, d), (d, tokens), *[(chunks, tokens, CHUNK)] * 3)],
        in_specs=[ANY] * 8,
        out_specs=[VMEM] * 3 + [ANY] * 5,
        scratch_shapes=[
            *(pltpu.VMEM(s, BF16) for s in ((d, ff), (d, ff), (ff, d), (tokens, d))),
            pltpu.VMEM((slots, 2, d, CHUNK), F32),
            pltpu.VMEM((ff, d), F32),
            *Scatter.scratch(side, rows, chunks * len(SUBS), stages * len(SUBS)),
            *Scatter.scratch(side, drows, d // LANES, d // LANES),
            *(dma(s) for s in ((2,), (2, tokens // SPAN), (3, chunks), (3, tokens // SPAN), (3,), (5, 2))),
        ],
        compiler_params=pltpu.CompilerParams(vmem_limit_bytes=VMEM_LIMIT, collective_id=1, has_side_effects=True),
        cost_estimate=pl.CostEstimate(flops=16 * tokens * d * ff, bytes_accessed=40 * tokens * d, transcendentals=tokens * ff),
    )(a1, a1t, dy, dyt, h, wg, wu, wd)


def back_kernel(side, slots, stages, dh, dht, a0t, po, ao, bo, wd, g1, u1, d1, gg, gu, gd, total, vd, vdh, vdht, vat, pair, ab, own, dwd, *rest):
    wide_refs, tall_refs, (tiles, lsem, asem, psem, tsem) = rest[:6], rest[6:12], rest[12:]
    t = Torus(side)
    tokens, d = vdh.shape
    ff = vd.shape[0]
    chunks, spans = ff // CHUNK, tokens // SPAN
    depth = ab.shape[1]
    grads = Grads(t, own, dwd, wide_refs, tall_refs, gg, gu, gd, slots, stages, 1)

    def saved(step):
        c, j, slot = step // spans, lax.rem(step, spans), lax.rem(step, depth)
        return [local(s.at[c, aligned(j * SPAN, SPAN)], ab.at[i, slot], asem.at[i, slot]) for i, s in enumerate((ao, bo))]

    def begin(copies):
        for c in copies:
            c.start()

    def end(copies):
        for c in copies:
            c.wait()

    ins = [local(s, o, lsem.at[i]) for i, (s, o) in enumerate(((dht, vdht), (dh, vdh), (a0t, vat), (wd, vd)))]
    ins[0].start()
    for c in range(2):
        fetch(po, pair, psem, c).start()
    t.greet(greeted(t, range(1, side)))
    ins[0].wait()

    def gradient(c):
        @pl.when(c == 1)
        def _():
            begin(ins[1:])

        for step in range(depth - 1):

            @pl.when(c == 2 + step)
            def _(step=step):
                begin(saved(step))

        grads.tall_gradient(c, chunks, vdht, po, pair, psem)

    loop(chunks, gradient)
    end(ins[1:])

    def hidden(c):
        cols = aligned(c * CHUNK, CHUNK)

        def span(j):
            step = c * spans + j

            @pl.when(step + depth - 1 < chunks * spans)
            def _():
                begin(saved(step + depth - 1))

            end(saved(step))
            slot = lax.rem(step, depth)
            for u in range(UNROLL):
                r = aligned(j * SPAN + u * TILE, TILE)
                mine = pl.ds(u * TILE, TILE)
                dp = rounded(dot_nt(vdh[r, :], vd[cols, :]))
                for i in BOTH:
                    pair[i, r, :] = (dp * ab[i, slot, mine, :]).astype(BF16)

        loop(spans, span)

        grads.tall_pairs(c, d // CHUNK, range(5))

        slot = lax.rem(c, slots)
        for which in BOTH:
            own[slot, which] = dot(vat[...], pair[which])
        grads.earlier((1, 2, 3, 4), c)
        grads.wide_stage(0, c)

    loop(chunks, hidden)
    for first in (1, 2, 3, 4):
        for back, n in enumerate(range(first, 5), 1):
            grads.wide_stage(n, chunks - back)

    squares = functools.reduce(lambda a, b: a + b, [jnp.sum(jnp.square(g[...].astype(F32))) for g in (g1, u1, d1, gg, gu, gd)])
    value = jnp.full(total.shape, squares, F32)
    for axis in BOTH:
        tiles[axis, 0] = value
        sent = [remote(tiles.at[axis, 0], tiles.at[axis, away], tsem.at[axis, 0, away], tsem.at[axis, 1, away], t.id(axis, away)) for away in range(1, side)]
        begin(sent)
        end(sent)
        value = functools.reduce(lambda a, b: a + b, [tiles[axis, i] for i in range(side)])
    total[...] = value


def back(side, dh, dht, a0t, po, ao, bo, wd, g1, u1, d1):
    tokens, d = dh.shape
    ff = wd.shape[0]
    rows, drows = g1.shape[0], d1.shape[0]
    chunks = ff // CHUNK
    slots, stages, depth = 3, 4, 5
    shape = jax.ShapeDtypeStruct
    dma = pltpu.SemaphoreType.DMA
    return pl.pallas_call(
        functools.partial(back_kernel, side, slots, stages),
        name="back",
        out_shape=[shape((rows, ff), BF16), shape((rows, ff), BF16), shape((drows, d), BF16), shape((8, LANES), F32)],
        in_specs=[ANY] * 7 + [VMEM] * 3,
        out_specs=[VMEM] * 4,
        scratch_shapes=[
            *(pltpu.VMEM(s, BF16) for s in ((ff, d), (tokens, d), (d, tokens), (d, tokens), (3, tokens, CHUNK))),
            pltpu.VMEM((2, depth, SPAN, CHUNK), F32),
            pltpu.VMEM((slots, 2, d, CHUNK), F32),
            pltpu.VMEM((ff, d), F32),
            *Scatter.scratch(side, rows, chunks * len(SUBS), stages * len(SUBS)),
            *Scatter.scratch(side, drows, d // LANES, d // LANES),
            pltpu.VMEM((2, side, 8, LANES), F32),
            *(dma(s) for s in ((4,), (2, depth), (3,), (2, 2, side))),
        ],
        compiler_params=pltpu.CompilerParams(vmem_limit_bytes=VMEM_LIMIT, collective_id=2, has_side_effects=True),
        cost_estimate=pl.CostEstimate(flops=8 * tokens * d * ff, bytes_accessed=40 * tokens * d, transcendentals=0),
    )(dh, dht, a0t, po, ao, bo, wd, g1, u1, d1)


def adamw(w, m, v, g):
    m = 0.9 * m + 0.1 * g
    v = 0.95 * v + 0.05 * g * g
    step = m * lax.rsqrt(v + 1e-8) + 0.1 * w
    return (w - 0.02 * step).astype(BF16), m, v


def step_kernel(count, total, *refs):
    ws, ms, vs, firsts, seconds = (refs[i : i + 3] for i in range(0, 15, 3))
    outs = refs[15:]
    factor = jnp.minimum(1.0, 0.5 * lax.rsqrt(total[0:1, 0:1] / count + 1e-30))
    for i, (w, m, v, first, second) in enumerate(zip(ws, ms, vs, firsts, seconds)):
        for layer, g in enumerate((first, second)):
            new = adamw(w[layer].astype(F32), m[layer], v[layer], g[...].astype(F32) * factor)
            for which, value in enumerate(new):
                outs[3 * which + i][layer] = value


def updated(count, total, weights, m, v, firsts, seconds):
    shape = jax.ShapeDtypeStruct
    outs = [shape(w.shape, dtype) for dtype in (BF16, F32, F32) for w in weights]
    return pl.pallas_call(
        functools.partial(step_kernel, count),
        name="adamw",
        out_shape=outs,
        in_specs=[VMEM] * 16,
        out_specs=[VMEM] * len(outs),
        compiler_params=pltpu.CompilerParams(vmem_limit_bytes=VMEM_LIMIT // 2),
    )(total, *weights, *m, *v, *firsts, *seconds)


def solution(mesh):
    side = math.isqrt(mesh.shape["dp"])
    group = side * side

    def step(x, dy, *arrays):
        weights, m, v = (arrays[i : i + 3] for i in (0, 3, 6))
        wg, wu, wd = weights
        x, dy = x[0], dy[0]
        d, ff = x.shape[1], wg.shape[2]
        ao, bo, po, a0t, dyt, h, a1, a1t, wd0, wg1, wu1, wd1 = front(side, x, dy, wg, wu, wd)
        last = mid(side, wg.shape[1], wd.shape[1], a1, a1t, dy, dyt, h, wg1.reshape(d, ff), wu1.reshape(d, ff), wd1.reshape(ff, d))
        g1, dh, dht = last[:3], last[3], last[4]
        *g0, total = back(side, dh, dht, a0t, po, ao, bo, wd0.reshape(ff, d), *g1)
        count = group * sum(g.size for g in (*g0, *g1))
        return tuple(updated(count, total, weights, m, v, g0, g1))

    states, cut = P(("rep", "dp"), None, None), P(None, "dp", None)
    return jax.shard_map(
        step,
        mesh=mesh,
        in_specs=(states, states) + (cut,) * 9,
        out_specs=(P("rep", "dp", None),) * 9,
        check_vma=False,
    )
```
